256 devices in a mesh: rows: 64 (over z, y, core), cols: 4 (over x).
Axes of the slice: x: 4, y: 4, z: 8, core: 2. Of those that a mesh axis runs over, the one named last changes fastest.
Arguments:
- adjacency_tiles: bfloat16 [1536, 12, 128, 128], P(('rows', 'cols')), may hold values from 2.170139e-08 to 0.25
- col_block: int32 [1536, 12], P(('rows', 'cols')), may hold values from 0 to 1535, as said below
- label_prior: float32 [196608, 256], P(('rows', 'cols')), may hold values from 0.05 to 20.1
- seed_label: int32 [196608], P(('rows', 'cols')), may hold values from 0 to 255
- seed_mask: int32 [196608], P(('rows', 'cols')), may hold values 0 or 1
Outputs:
- labels: float32 [196608, 256], P(('rows', 'cols'))
The draws below stay inside these ranges and needn't reach their ends.
Inputs may be any that keep to these rules, and one draw needn't show every extreme that they name: Row block b is held by device b // 6 of rows+cols, whose rows group is b // (6 * 4). col_block[b, 0] = b. For each device, all its tiles that reference blocks of another rows group reference one and the same block of that group, and each device references every rows group.
All inputs are finite; a program needn't handle non-finite values. No bound on the sum of `seed_mask` on one device may be relied on, other than what follows from the above.
Results may differ from the reference program's by a relative error of at most 0.00041.
Values may be sent and summed in bfloat16 or wider, within the bound.
No kernel may reach another device: no remote copies, remote signals or barrier semaphores. Data moves between devices by JAX's collectives and lax.ppermute only.
A program may use at most 64 MiB of HBM per device.

```python
import jax
import jax.numpy as jnp
from jax import lax

CLASSES = 256
BLOCK = 128
DEGREE = 12
HOPS = 4
BLOCKS_DEV = 6
BLOCKS = 1536
NODES = 196608
N_ROWS = 64
N_COLS = 4


def draw_col_block(key, part):
    device_count = BLOCKS // BLOCKS_DEV
    group_size = N_COLS * BLOCKS_DEV
    slot_count = BLOCKS_DEV * (DEGREE - 1)

    def per_device(device):
        device_key = jax.random.fold_in(jax.random.fold_in(key, 7177), device)
        k_within, k_group, k_local, k_coin, k_perm = jax.random.split(device_key, 5)
        home_group = device // N_COLS
        chosen = jax.random.randint(k_within, (N_ROWS,), 0, group_size)
        extra_group = jax.random.randint(k_group, (slot_count - N_ROWS,), 0, N_ROWS)
        coin_flip = jax.random.randint(k_coin, (slot_count - N_ROWS,), 0, 2)
        extra_group = jnp.where(coin_flip == 0, home_group, extra_group)
        groups_all = jnp.concatenate([jnp.arange(N_ROWS, dtype=jnp.int32), extra_group.astype(jnp.int32)])
        local_pick = jax.random.randint(k_local, (slot_count,), 0, group_size)
        within_all = jnp.where(groups_all == home_group, local_pick, chosen[groups_all])
        shuffle = jax.random.permutation(k_perm, slot_count)
        picked = (groups_all * group_size + within_all)[shuffle].reshape(BLOCKS_DEV, DEGREE - 1)
        diagonal = device * BLOCKS_DEV + jnp.arange(BLOCKS_DEV, dtype=jnp.int32)
        return jnp.concatenate([diagonal[:, None], picked.astype(jnp.int32)], axis=1)
    result = jax.vmap(per_device)(jnp.arange(device_count, dtype=jnp.int32))
    return result.reshape(BLOCKS, DEGREE).astype(jnp.int32)


def draw_adjacency_tiles(key, part):
    k_scale, k_entry, k_pick = jax.random.split(jax.random.fold_in(key, 3301), 3)
    span = jnp.log(jnp.float32(100.0))
    tile_scale = jnp.exp(span * jax.random.uniform(k_scale, (BLOCKS, DEGREE), jnp.float32))
    tile_scale = tile_scale / jnp.sum(tile_scale, axis=1, keepdims=True)
    shape = (BLOCKS, DEGREE, BLOCK, BLOCK)
    entries = jnp.exp(jax.random.uniform(k_entry, shape, jnp.float32, jnp.log(0.5), jnp.log(2.0)))
    dominant = jax.random.randint(k_pick, shape, 0, 16) == 0
    pattern = jnp.where(dominant, entries * (16.0 / BLOCK), jnp.float32(0.01 / BLOCK))
    values = tile_scale[:, :, None, None] * pattern
    return values.astype(jnp.bfloat16)


def draw_label_prior(key, part):
    k_base, k_pick, k_boost = jax.random.split(jax.random.fold_in(key, 5407), 3)
    base = jnp.exp(jax.random.uniform(k_base, (NODES, CLASSES), jnp.float32, jnp.log(0.05), 0.0))
    picked = jax.random.randint(k_pick, (NODES, CLASSES), 0, 16) == 0
    boost = jnp.exp(3.0 * jax.random.uniform(k_boost, (NODES, CLASSES), jnp.float32))
    factor = jnp.where(picked, boost, jnp.float32(1.0))
    return (base * factor).astype(jnp.float32)


def with_ends(values, rng, low, high):
    spot = [jax.random.randint(jax.random.fold_in(rng, axis), (), 0, length) for axis, length in enumerate(values.shape)]
    main_axis = values.shape.index(max(values.shape))
    beside = spot[:main_axis] + [(spot[main_axis] + 1) % values.shape[main_axis]] + spot[main_axis + 1:]
    return values.at[tuple(spot)].set(low).at[tuple(beside)].set(high)


def setup_inputs(seed: int = 0) -> dict:
    seeds = jax.random.split(jax.random.key(seed), 6)
    adjacency_tiles = draw_adjacency_tiles(jax.random.fold_in(seeds[5], 71), 0)
    col_block = draw_col_block(jax.random.fold_in(seeds[5], 71), 0)
    label_prior = draw_label_prior(jax.random.fold_in(seeds[5], 71), 0)
    seed_label = with_ends(jax.random.randint(seeds[3], (NODES,), 0, CLASSES), jax.random.fold_in(seeds[3], 1), 0, CLASSES - 1).astype(jnp.int32)
    seed_mask = with_ends((jax.random.randint(seeds[4], (NODES,), 0, 4) < 1).astype(jnp.int32), jax.random.fold_in(seeds[4], 1), 0, 1)
    return {"adjacency_tiles": adjacency_tiles, "col_block": col_block, "label_prior": label_prior, "seed_label": seed_label, "seed_mask": seed_mask}


ALPHA = 0.85
SEED_BOOST = 8.0


def prepare(label_prior, seed_label, seed_mask):
    classes = label_prior.shape[1]
    one_hot = (seed_label[:, None] == jnp.arange(classes, dtype=jnp.int32)[None, :]).astype(jnp.float32)
    anchor_raw = label_prior + SEED_BOOST * seed_mask[:, None].astype(jnp.float32) * one_hot
    return anchor_raw * (classes / jnp.sum(anchor_raw, axis=1, keepdims=True))


def reference(adjacency_tiles, col_block, label_prior, seed_label, seed_mask):
    anchor = prepare(label_prior, seed_label, seed_mask)
    labels = anchor
    for hop_index in range(HOPS):
        sent_blocks = labels.astype(jnp.bfloat16).reshape(BLOCKS, BLOCK, CLASSES)

        def per_block(pair_in):
            tile_set, col_ids = pair_in
            operand = sent_blocks[col_ids]
            return jnp.einsum("kij,kjc->ic", tile_set.astype(jnp.float32), operand.astype(jnp.float32))

        spread = lax.map(per_block, (adjacency_tiles, col_block), batch_size=16).reshape(NODES, CLASSES)
        blended = ALPHA * spread + (1.0 - ALPHA) * anchor
        labels = blended * (CLASSES / jnp.sum(blended, axis=1, keepdims=True))
    return labels
```

```python
import functools

import jax
import jax.numpy as jnp
from jax import lax
from jax.experimental import pallas as pl
from jax.experimental.pallas import tpu as pltpu
from jax.sharding import PartitionSpec as P

HOPS = 4
PARTS = 2


ALPHA = 0.85
SEED_BOOST = 8.0

ANY = pl.BlockSpec(memory_space=pl.ANY)
VMEM = pl.BlockSpec(memory_space=pltpu.VMEM)
SMEM = pl.BlockSpec(memory_space=pltpu.SMEM)


def prepare(label_prior, seed_label, seed_mask):
    classes = label_prior.shape[1]
    one_hot = (seed_label[:, None] == jnp.arange(classes, dtype=jnp.int32)[None, :]).astype(
        jnp.float32
    )
    anchor_raw = label_prior + SEED_BOOST * seed_mask[:, None].astype(jnp.float32) * one_hot
    return anchor_raw * (classes / jnp.sum(anchor_raw, axis=1, keepdims=True))


def ask_blocks(owner_group, within, own_group, n_rows):
    group_ids = jnp.arange(n_rows, dtype=jnp.int32)
    matched = owner_group.reshape(-1)[:, None] == group_ids[None, :]
    wanted = jnp.max(jnp.where(matched, within.reshape(-1)[:, None], 0), axis=0)
    wanted = jnp.where(group_ids == own_group, 0, wanted)
    return lax.all_to_all(
        wanted.reshape(n_rows, 1), "rows", split_axis=0, concat_axis=0, tiled=True
    )


def reply_kernel(asked_ref, *refs, n_cols):
    parts, out_ref, table, in_sems, out_sem = refs[:n_cols], refs[n_cols], *refs[n_cols + 1 :]
    blocks_dev = parts[0].shape[0]
    n = out_ref.shape[0]
    loads = [
        pltpu.make_async_copy(p, table.at[pl.ds(i * blocks_dev, blocks_dev)], in_sems.at[i])
        for i, p in enumerate(parts)
    ]
    for c in loads:
        c.start()
    for c in loads:
        c.wait()

    @pl.loop(0, n)
    def _(i):
        pltpu.make_async_copy(table.at[asked_ref[i]], out_ref.at[i], out_sem).start()

    pltpu.make_async_copy(out_ref, out_ref, out_sem).wait()


def reply_blocks(asked, parts):
    blocks_dev, block, width = parts[0].shape
    n = asked.shape[0]
    n_cols = len(parts)
    size = block * width * 2
    return pl.pallas_call(
        functools.partial(reply_kernel, n_cols=n_cols),
        out_shape=jax.ShapeDtypeStruct((n, block, width), jnp.bfloat16),
        in_specs=[SMEM] + [ANY] * n_cols,
        out_specs=ANY,
        scratch_shapes=[
            pltpu.VMEM((n_cols * blocks_dev, block, width), jnp.bfloat16),
            pltpu.SemaphoreType.DMA((n_cols,)),
            pltpu.SemaphoreType.DMA,
        ],
        cost_estimate=pl.CostEstimate(
            flops=4_000_000, bytes_accessed=(n + n_cols * blocks_dev) * size, transcendentals=0
        ),
        name="reply",
    )(asked, *parts)


def spread_kernel(index_ref, tiles_ref, weight_ref, anchor_ref, *refs, n_src):
    sources, out_ref, table, sems = refs[:n_src], refs[n_src], *refs[n_src + 1 :]
    blocks_dev, degree, block, _ = tiles_ref.shape
    loads, at = [], 0
    for i, s in enumerate(sources):
        loads.append(pltpu.make_async_copy(s, table.at[pl.ds(at, s.shape[0])], sems.at[i]))
        at += s.shape[0]
    for c in loads:
        c.start()
    for c in loads:
        c.wait()

    @pl.loop(0, blocks_dev)
    def _(b):
        total = None
        for k in range(0, degree, 2):
            left = jnp.concatenate([tiles_ref[b, k], tiles_ref[b, k + 1]], axis=1)
            right = jnp.concatenate(
                [table[index_ref[b * degree + k]], table[index_ref[b * degree + k + 1]]], axis=0
            )
            term = jnp.dot(left, right, preferred_element_type=jnp.float32)
            total = term if total is None else total + term
        rows = pl.ds(pl.multiple_of(b * block, block), block)
        out_ref[rows, :] = (weight_ref[rows, :] * total + anchor_ref[rows, :]).astype(out_ref.dtype)


def spread_blocks(index, tiles, weight, anchor, sources, dtype):
    blocks_dev, degree, block, _ = tiles.shape
    width = anchor.shape[1]
    n_src = len(sources)
    total = sum(s.shape[0] for s in sources)
    return pl.pallas_call(
        functools.partial(spread_kernel, n_src=n_src),
        out_shape=jax.ShapeDtypeStruct((blocks_dev * block, width), dtype),
        in_specs=[SMEM, VMEM, VMEM, VMEM] + [ANY] * n_src,
        out_specs=VMEM,
        scratch_shapes=[
            pltpu.VMEM((total, block, width), jnp.bfloat16),
            pltpu.SemaphoreType.DMA((n_src,)),
        ],
        cost_estimate=pl.CostEstimate(
            flops=2 * blocks_dev * degree * block * block * width,
            bytes_accessed=total * block * width * 2 + tiles.size * 2,
            transcendentals=0,
        ),
        name="spread",
    )(index, tiles, weight, anchor, *sources)


def local(adjacency_tiles, col_block, label_prior, seed_label, seed_mask):
    blocks_dev, degree, block, _ = adjacency_tiles.shape
    classes = label_prior.shape[1]
    width = classes // PARTS
    n_rows = lax.axis_size("rows")
    n_cols = lax.axis_size("cols")
    group_size = n_cols * blocks_dev
    own_group = lax.axis_index("rows")
    own_col = lax.axis_index("cols")
    owner_group = col_block // group_size
    within = col_block % group_size

    def from_here(w):
        return (w // blocks_dev + n_cols - own_col) % n_cols * blocks_dev + w % blocks_dev

    index = jnp.where(
        owner_group == own_group, from_here(within), group_size + owner_group
    ).reshape(-1)
    asked = from_here(ask_blocks(owner_group, within, own_group, n_rows)[:, 0])
    anchor = prepare(label_prior, seed_label, seed_mask)

    row_sum = jnp.sum(adjacency_tiles.astype(jnp.float32), axis=(1, 3)).reshape(-1, 1)
    scale = 1.0 / (ALPHA * row_sum + (1.0 - ALPHA))
    weight = jnp.broadcast_to(ALPHA * scale, (blocks_dev * block, width))

    ranges = [slice(p * width, (p + 1) * width) for p in range(PARTS)]
    anchors = [(1.0 - ALPHA) * scale * anchor[:, r] for r in ranges]
    sent = [anchor[:, r].astype(jnp.bfloat16) for r in ranges]
    blended = [None] * PARTS
    for hop in range(HOPS):
        last = hop == HOPS - 1
        for p in range(PARTS):
            own = sent[p].reshape(blocks_dev, block, width)
            parts = [own] + [
                lax.ppermute(own, "cols", [((x + d) % n_cols, x) for x in range(n_cols)])
                for d in range(1, n_cols)
            ]
            reply = reply_blocks(asked, parts)
            remote = lax.all_to_all(reply, "rows", split_axis=0, concat_axis=0, tiled=True)
            blended[p] = spread_blocks(
                index, adjacency_tiles, weight, anchors[p], parts + [remote],
                jnp.float32 if last else jnp.bfloat16,
            )
        sent = blended
    labels = jnp.concatenate(blended, axis=1)
    return labels * (classes / jnp.sum(labels, axis=1, keepdims=True))


def solution(mesh):
    in_specs = (
        P(("rows", "cols"), None, None, None),
        P(("rows", "cols"), None),
        P(("rows", "cols"), None),
        P(("rows", "cols")),
        P(("rows", "cols")),
    )
    out_specs = P(("rows", "cols"), None)
    return jax.shard_map(local, mesh=mesh, in_specs=in_specs, out_specs=out_specs, check_vma=False)
```

```python
import functools

import jax
import jax.numpy as jnp
from jax import lax
from jax.experimental import pallas as pl
from jax.experimental.pallas import tpu as pltpu
from jax.sharding import Mesh
from jax.sharding import PartitionSpec as P

HOPS = 4
PARTS = 2
AXES = ("zy", "core", "x")
GROUP = ("zy", "core")


ALPHA = 0.85
SEED_BOOST = 8.0

ANY = pl.BlockSpec(memory_space=pl.ANY)
VMEM = pl.BlockSpec(memory_space=pltpu.VMEM)
SMEM = pl.BlockSpec(memory_space=pltpu.SMEM)
HBM = pl.BlockSpec(memory_space=pltpu.HBM)


def prepare(label_prior, seed_label, seed_mask):
    classes = label_prior.shape[1]
    one_hot = (seed_label[:, None] == jnp.arange(classes, dtype=jnp.int32)[None, :]).astype(
        jnp.float32
    )
    anchor_raw = label_prior + SEED_BOOST * seed_mask[:, None].astype(jnp.float32) * one_hot
    return anchor_raw * (classes / jnp.sum(anchor_raw, axis=1, keepdims=True))


def ask_blocks(owner_group, place, own_group, n_rows):
    group_ids = jnp.arange(n_rows, dtype=jnp.int32)
    matched = owner_group.reshape(-1)[:, None] == group_ids[None, :]
    wanted = jnp.max(jnp.where(matched, place.reshape(-1)[:, None], 0), axis=0)
    wanted = jnp.where(group_ids == own_group, 0, wanted)
    return lax.all_to_all(wanted.reshape(n_rows, 1), GROUP, 0, 0, tiled=True)[:, 0]


def reply_kernel(asked_ref, *refs, n_cols):
    parts, out_ref, table, in_sems, out_sem = refs[:n_cols], refs[n_cols], *refs[n_cols + 1 :]
    blocks_dev = parts[0].shape[0]
    n = out_ref.shape[0]
    loads = [
        pltpu.make_async_copy(p, table.at[pl.ds(i * blocks_dev, blocks_dev)], in_sems.at[i])
        for i, p in enumerate(parts)
    ]
    for c in loads:
        c.start()
    for c in loads:
        c.wait()

    @pl.loop(0, n)
    def _(i):
        pltpu.make_async_copy(table.at[asked_ref[i]], out_ref.at[i], out_sem).start()

    pltpu.make_async_copy(out_ref, out_ref, out_sem).wait()


def reply_blocks(asked, parts):
    blocks_dev, block, width = parts[0].shape
    n = asked.shape[0]
    n_cols = len(parts)
    size = block * width * 2
    return pl.pallas_call(
        functools.partial(reply_kernel, n_cols=n_cols),
        out_shape=jax.ShapeDtypeStruct((n, block, width), jnp.bfloat16),
        in_specs=[SMEM] + [ANY] * n_cols,
        out_specs=ANY,
        scratch_shapes=[
            pltpu.VMEM((n_cols * blocks_dev, block, width), jnp.bfloat16),
            pltpu.SemaphoreType.DMA((n_cols,)),
            pltpu.SemaphoreType.DMA,
        ],
        cost_estimate=pl.CostEstimate(
            flops=4_000_000, bytes_accessed=(n + n_cols * blocks_dev) * size, transcendentals=0
        ),
        name="reply",
    )(asked, *parts)


def spread_kernel(index_ref, core_ref, tiles_ref, weight_ref, anchor_ref, *refs, n_src, final):
    sources, same_ref, other_ref = refs[:n_src], refs[n_src], refs[n_src + 1]
    first_ref = refs[n_src + 2] if final else None
    out_ref, table, sems = refs[-3:]
    blocks_dev, degree, block, _ = tiles_ref.shape
    width = anchor_ref.shape[1]
    loads, at = [], 0
    for i, s in enumerate([*sources, same_ref.at[:, core_ref[0]], other_ref.at[:, core_ref[0]]]):
        loads.append(pltpu.make_async_copy(s, table.at[pl.ds(at, s.shape[0])], sems.at[i]))
        at += s.shape[0]
    for c in loads:
        c.start()
    for c in loads:
        c.wait()

    @pl.loop(0, blocks_dev)
    def _(b):
        left = jnp.concatenate([tiles_ref[b, k] for k in range(degree)], axis=1)
        right = jnp.concatenate(
            [table[index_ref[b * degree + k]] for k in range(degree)], axis=0
        )
        total = jnp.dot(left, right, preferred_element_type=jnp.float32)
        rows = pl.ds(pl.multiple_of(b * block, block), block)
        blended = weight_ref[rows, :] * total + anchor_ref[rows, :]
        if not final:
            out_ref[rows, :] = blended.astype(out_ref.dtype)
        else:
            first = first_ref[rows, :]
            classes = 2 * width
            factor = classes / jnp.sum(first + blended, axis=1, keepdims=True)
            out_ref[rows, :width] = first * factor
            out_ref[rows, width:] = blended * factor


def spread_blocks(index, core, tiles, weight, anchor, pieces, same, other, dtype, first=None):
    blocks_dev, degree, block, _ = tiles.shape
    width = anchor.shape[1]
    final = first is not None
    n_src = len(pieces)
    total = sum(s.shape[0] for s in pieces) + same.shape[0] + other.shape[0]
    return pl.pallas_call(
        functools.partial(spread_kernel, n_src=n_src, final=final),
        out_shape=jax.ShapeDtypeStruct((blocks_dev * block, width * (2 if final else 1)), dtype),
        in_specs=[SMEM, SMEM, VMEM, VMEM, VMEM] + [ANY] * n_src + [HBM, HBM] + [VMEM] * final,
        out_specs=VMEM,
        scratch_shapes=[
            pltpu.VMEM((total, block, width), jnp.bfloat16),
            pltpu.SemaphoreType.DMA((n_src + 2,)),
        ],
        cost_estimate=pl.CostEstimate(
            flops=2 * blocks_dev * degree * block * block * width,
            bytes_accessed=total * block * width * 2 + tiles.size * 2,
            transcendentals=0,
        ),
        name="spread",
    )(index, core, tiles, weight, anchor, *pieces, same, other, *([first] if final else []))


def local(adjacency_tiles, col_block, label_prior, seed_label, seed_mask):
    blocks_dev, degree, block, _ = adjacency_tiles.shape
    classes = label_prior.shape[1]
    width = classes // PARTS
    n_rows = lax.axis_size(GROUP)
    n_cols = lax.axis_size("x")
    n_chips = lax.axis_size("zy")
    group_size = n_cols * blocks_dev
    own_group = lax.axis_index(GROUP)
    own_col = lax.axis_index("x")
    own_core = lax.axis_index("core")
    owner_group = col_block // group_size
    within = col_block % group_size

    place = (within // blocks_dev + n_cols - own_col) % n_cols * blocks_dev + within % blocks_dev
    chip, core = owner_group // 2, owner_group % 2
    slot = group_size + chip + jnp.where(core == own_core, 0, n_chips)
    index = jnp.where(owner_group == own_group, place, slot).reshape(-1)
    asked = ask_blocks(owner_group, place, own_group, n_rows)
    anchor = prepare(label_prior, seed_label, seed_mask)

    row_sum = jnp.sum(adjacency_tiles.astype(jnp.float32), axis=(1, 3)).reshape(-1, 1)
    scale = 1.0 / (ALPHA * row_sum + (1.0 - ALPHA))
    weight = jnp.broadcast_to(ALPHA * scale, (blocks_dev * block, width))

    ranges = [slice(p * width, (p + 1) * width) for p in range(PARTS)]
    anchors = [(1.0 - ALPHA) * scale * anchor[:, r] for r in ranges]
    blended = [anchor[:, r].astype(jnp.bfloat16) for r in ranges]
    for hop in range(HOPS):
        last = hop == HOPS - 1
        for p in range(PARTS):
            own = blended[p].reshape(blocks_dev, block, width)
            pieces = [own] + [
                lax.ppermute(own, "x", [((x + d) % n_cols, x) for x in range(n_cols)])
                for d in range(1, n_cols)
            ]
            reply = reply_blocks(asked, pieces).reshape(n_chips, 2, block, width)
            same = lax.all_to_all(reply, "zy", 0, 0, tiled=True)
            other = lax.ppermute(same, "core", [(0, 1), (1, 0)])
            blended[p] = spread_blocks(
                index, own_core.reshape(1), adjacency_tiles, weight, anchors[p], pieces,
                same, other,
                jnp.float32 if last else jnp.bfloat16,
                blended[0] if last and p == 1 else None,
            )
    return blended[1]


def solution(mesh):
    n_rows, n_cols = mesh.devices.shape
    fine = Mesh(mesh.devices.reshape(n_rows // 2, 2, n_cols), AXES)
    in_specs = (
        P(AXES, None, None, None),
        P(AXES, None),
        P(AXES, None),
        P(AXES),
        P(AXES),
    )
    out_specs = P(AXES, None)
    return jax.shard_map(local, mesh=fine, in_specs=in_specs, out_specs=out_specs, check_vma=False)
```

```python
import functools

import jax
import jax.numpy as jnp
from jax import lax
from jax.experimental import pallas as pl
from jax.experimental.pallas import tpu as pltpu
from jax.sharding import Mesh
from jax.sharding import PartitionSpec as P

HOPS = 4
PARTS = 2
AXES = ("zy", "core", "x")
GROUP = ("zy", "core")
LANES = 128


ALPHA = 0.85
SEED_BOOST = 8.0

ANY = pl.BlockSpec(memory_space=pl.ANY)
VMEM = pl.BlockSpec(memory_space=pltpu.VMEM)
SMEM = pl.BlockSpec(memory_space=pltpu.SMEM)
HBM = pl.BlockSpec(memory_space=pltpu.HBM)


def ask_blocks(owner_group, place, own_group, n_rows):
    group_ids = jnp.arange(n_rows, dtype=jnp.int32)
    matched = owner_group.reshape(-1)[:, None] == group_ids[None, :]
    wanted = jnp.max(jnp.where(matched, place.reshape(-1)[:, None], 0), axis=0)
    wanted = jnp.where(group_ids == own_group, 0, wanted).reshape(n_rows // 2, 2)
    own_core = lax.axis_index("core")
    other = lax.ppermute(wanted, "core", [(0, 1), (1, 0)])
    lane = jnp.arange(LANES, dtype=jnp.int32)[None, :]
    mine = jnp.where(own_core == 0, wanted[:, :1], wanted[:, 1:])
    others = jnp.where(own_core == 0, other[:, :1], other[:, 1:])
    rows = jnp.where(lane % 2 == own_core, mine, others)
    return lax.all_to_all(rows, "zy", 0, 0, tiled=True)


def prepare_kernel(prior_ref, label_ref, mask_ref, anchor_ref, *sent_refs):
    nodes, classes = prior_ref.shape
    width = sent_refs[0].shape[1]

    @pl.loop(0, nodes // LANES)
    def _(b):
        rows = pl.ds(pl.multiple_of(b * LANES, LANES), LANES)
        label = jnp.broadcast_to(label_ref[rows][None, :], (LANES, LANES)).T
        boost = SEED_BOOST * jnp.broadcast_to(
            mask_ref[rows][None, :].astype(jnp.float32), (LANES, LANES)
        ).T
        lane = lax.broadcasted_iota(jnp.int32, (LANES, LANES), 1)
        raw = [
            prior_ref[rows, at : at + LANES] + jnp.where(label == lane + at, boost, 0.0)
            for at in range(0, classes, LANES)
        ]
        raw = jnp.concatenate(raw, axis=1)
        anchor = raw * (classes / jnp.sum(raw, axis=1, keepdims=True))
        anchor_ref[rows, :] = anchor
        for i, s in enumerate(sent_refs):
            s[rows, :] = anchor[:, i * width : (i + 1) * width].astype(jnp.bfloat16)


def prepare(label_prior, seed_label, seed_mask):
    nodes, classes = label_prior.shape
    sent = jax.ShapeDtypeStruct((nodes, classes // PARTS), jnp.bfloat16)
    anchor, *sent = pl.pallas_call(
        prepare_kernel,
        out_shape=[jax.ShapeDtypeStruct((nodes, classes), jnp.float32)] + [sent] * PARTS,
        in_specs=[VMEM, VMEM, VMEM],
        out_specs=[VMEM] * (1 + PARTS),
        cost_estimate=pl.CostEstimate(
            flops=8 * nodes * classes, bytes_accessed=10 * nodes * classes, transcendentals=0
        ),
        name="prepare",
    )(label_prior, seed_label, seed_mask)
    return anchor, sent


def reply_kernel(asked_ref, *refs, n_cols):
    parts, out_ref, table, in_sems, out_sem = refs[:n_cols], refs[n_cols], *refs[n_cols + 1 :]
    blocks_dev = parts[0].shape[0]
    n = out_ref.shape[0]
    loads = [
        pltpu.make_async_copy(p, table.at[pl.ds(i * blocks_dev, blocks_dev)], in_sems.at[i])
        for i, p in enumerate(parts)
    ]
    for c in loads:
        c.start()
    for c in loads:
        c.wait()

    @pl.loop(0, n // 2)
    def _(chip):
        for core in range(2):
            pltpu.make_async_copy(
                table.at[asked_ref[chip, core]], out_ref.at[2 * chip + core], out_sem
            ).start()

    pltpu.make_async_copy(out_ref, out_ref, out_sem).wait()


def reply_blocks(asked, parts):
    blocks_dev, block, width = parts[0].shape
    n = 2 * asked.shape[0]
    n_cols = len(parts)
    size = block * width * 2
    return pl.pallas_call(
        functools.partial(reply_kernel, n_cols=n_cols),
        out_shape=jax.ShapeDtypeStruct((n, block, width), jnp.bfloat16),
        in_specs=[SMEM] + [HBM] * n_cols,
        out_specs=ANY,
        scratch_shapes=[
            pltpu.VMEM((n_cols * blocks_dev, block, width), jnp.bfloat16),
            pltpu.SemaphoreType.DMA((n_cols,)),
            pltpu.SemaphoreType.DMA,
        ],
        cost_estimate=pl.CostEstimate(
            flops=4_000_000, bytes_accessed=(n + n_cols * blocks_dev) * size, transcendentals=0
        ),
        name="reply",
    )(asked, *parts)


def spread_kernel(index_ref, core_ref, tiles_ref, weight_ref, anchor_ref, *refs, n_src, final):
    sources = [s if len(s.shape) == 3 else s.at[:, core_ref[0]] for s in refs[:n_src]]
    first_ref = refs[n_src] if final else None
    out_ref, table, sems = refs[-3:]
    blocks_dev, degree, block, _ = tiles_ref.shape
    width = anchor_ref.shape[1]
    loads, at = [], 0
    for i, s in enumerate(sources):
        loads.append(pltpu.make_async_copy(s, table.at[pl.ds(at, s.shape[0])], sems.at[i]))
        at += s.shape[0]
    for c in loads:
        c.start()
    for c in loads:
        c.wait()

    def row_block(b):
        left = jnp.concatenate([tiles_ref[b, k] for k in range(degree)], axis=1)
        right = jnp.concatenate(
            [table[index_ref[b * degree + k]] for k in range(degree)], axis=0
        )
        total = jnp.dot(left, right, preferred_element_type=jnp.float32)
        rows = pl.ds(b * block if final else pl.multiple_of(b * block, block), block)
        blended = weight_ref[rows, :] * total + anchor_ref[rows, :]
        if not final:
            out_ref[rows, :] = blended.astype(out_ref.dtype)
        else:
            first = first_ref[rows, :]
            classes = 2 * width
            factor = classes / jnp.sum(first + blended, axis=1, keepdims=True)
            out_ref[rows, :width] = first * factor
            out_ref[rows, width:] = blended * factor

    if final:
        for b in range(blocks_dev):
            row_block(b)
    else:
        pl.loop(0, blocks_dev)(row_block)


def spread_blocks(index, core, tiles, weight, anchor, sources, dtype, first=None):
    blocks_dev, degree, block, _ = tiles.shape
    width = anchor.shape[1]
    final = first is not None
    n_src = len(sources)
    total = sum(s.shape[0] for s in sources)
    places = [ANY if len(s.shape) == 3 else HBM for s in sources]
    return pl.pallas_call(
        functools.partial(spread_kernel, n_src=n_src, final=final),
        out_shape=jax.ShapeDtypeStruct((blocks_dev * block, width * (2 if final else 1)), dtype),
        in_specs=[SMEM, SMEM, VMEM, VMEM, VMEM] + places + [VMEM] * final,
        out_specs=VMEM,
        scratch_shapes=[
            pltpu.VMEM((total, block, width), jnp.bfloat16),
            pltpu.SemaphoreType.DMA((n_src,)),
        ],
        cost_estimate=pl.CostEstimate(
            flops=2 * blocks_dev * degree * block * block * width,
            bytes_accessed=total * block * width * 2 + tiles.size * 2,
            transcendentals=0,
        ),
        name="spread",
    )(index, core, tiles, weight, anchor, *sources, *([first] if final else []))


def local(adjacency_tiles, col_block, label_prior, seed_label, seed_mask):
    blocks_dev, _, block, _ = adjacency_tiles.shape
    classes = label_prior.shape[1]
    width = classes // PARTS
    n_rows = lax.axis_size(GROUP)
    n_cols = lax.axis_size("x")
    n_chips = lax.axis_size("zy")
    group_size = n_cols * blocks_dev
    own_group = lax.axis_index(GROUP)
    own_col = lax.axis_index("x")
    own_core = lax.axis_index("core")
    owner_group = col_block // group_size
    within = col_block % group_size

    place = (within // blocks_dev + n_cols - own_col) % n_cols * blocks_dev + within % blocks_dev
    chip, core = owner_group // 2, owner_group % 2
    slot = group_size + chip + jnp.where(core == own_core, 0, n_chips)
    index = jnp.where(owner_group == own_group, place, slot).reshape(-1)
    index_last = jnp.where(owner_group == own_group, place, group_size + owner_group).reshape(-1)
    asked = ask_blocks(owner_group, place, own_group, n_rows)
    anchor, blended = prepare(label_prior, seed_label, seed_mask)

    row_sum = jnp.sum(adjacency_tiles.astype(jnp.float32), axis=(1, 3)).reshape(-1, 1)
    scale = 1.0 / (ALPHA * row_sum + (1.0 - ALPHA))
    weight = jnp.broadcast_to(ALPHA * scale, (blocks_dev * block, width))

    ranges = [slice(p * width, (p + 1) * width) for p in range(PARTS)]
    anchors = [(1.0 - ALPHA) * scale * anchor[:, r] for r in ranges]
    for hop in range(HOPS):
        last = hop == HOPS - 1
        for p in range(PARTS):
            own = blended[p].reshape(blocks_dev, block, width)
            pieces = [own] + [
                lax.ppermute(own, "x", [((x + d) % n_cols, x) for x in range(n_cols)])
                for d in range(1, n_cols)
            ]
            reply = reply_blocks(asked, pieces)
            if last and p == PARTS - 1:
                remote = [lax.all_to_all(reply, GROUP, 0, 0, tiled=True)]
            else:
                reply = reply.reshape(n_chips, 2, block, width)
                same = lax.all_to_all(reply, "zy", 0, 0, tiled=True)
                remote = [same, lax.ppermute(same, "core", [(0, 1), (1, 0)])]
            blended[p] = spread_blocks(
                index_last if len(remote) == 1 else index,
                own_core.reshape(1), adjacency_tiles, weight, anchors[p], pieces + remote,
                jnp.float32 if last else jnp.bfloat16,
                blended[0] if last and p == PARTS - 1 else None,
            )
    return blended[1]


def solution(mesh):
    n_rows, n_cols = mesh.devices.shape
    fine = Mesh(mesh.devices.reshape(n_rows // 2, 2, n_cols), AXES)
    in_specs = (
        P(AXES, None, None, None),
        P(AXES, None),
        P(AXES, None),
        P(AXES),
        P(AXES),
    )
    out_specs = P(AXES, None)

    return jax.shard_map(local, mesh=fine, in_specs=in_specs, out_specs=out_specs, check_vma=False)
```

```python
import functools

import jax
import jax.numpy as jnp
from jax import lax
from jax.experimental import pallas as pl
from jax.experimental.pallas import tpu as pltpu
from jax.sharding import Mesh
from jax.sharding import PartitionSpec as P

HOPS = 4
HOLD = {(0, 0): 2100, (1, 0): 700, (1, 1): 600, (2, 0): 700, (2, 1): 600, (3, 0): 700}
PARTS = 2
AXES = ("zy", "core", "x")
GROUP = ("zy", "core")
LANES = 128


ALPHA = 0.85
SEED_BOOST = 8.0

ANY = pl.BlockSpec(memory_space=pl.ANY)
VMEM = pl.BlockSpec(memory_space=pltpu.VMEM)
SMEM = pl.BlockSpec(memory_space=pltpu.SMEM)
HBM = pl.BlockSpec(memory_space=pltpu.HBM)


def ask_blocks(owner_group, place, own_group, n_rows):
    group_ids = jnp.arange(n_rows, dtype=jnp.int32)
    matched = owner_group.reshape(-1)[:, None] == group_ids[None, :]
    wanted = jnp.max(jnp.where(matched, place.reshape(-1)[:, None], 0), axis=0)
    wanted = jnp.where(group_ids == own_group, 0, wanted).reshape(n_rows // 2, 2)
    own_core = lax.axis_index("core")
    other = lax.ppermute(wanted, "core", [(0, 1), (1, 0)])
    lane = jnp.arange(LANES, dtype=jnp.int32)[None, :]
    mine = jnp.where(own_core == 0, wanted[:, :1], wanted[:, 1:])
    others = jnp.where(own_core == 0, other[:, :1], other[:, 1:])
    rows = jnp.where(lane % 2 == own_core, mine, others)
    return lax.all_to_all(rows, "zy", 0, 0, tiled=True)


def prepare_kernel(prior_ref, label_ref, mask_ref, anchor_ref, *sent_refs):
    nodes, classes = prior_ref.shape
    width = sent_refs[0].shape[1]

    @pl.loop(0, nodes // LANES)
    def _(b):
        rows = pl.ds(pl.multiple_of(b * LANES, LANES), LANES)
        label = jnp.broadcast_to(label_ref[rows][None, :], (LANES, LANES)).T
        boost = SEED_BOOST * jnp.broadcast_to(
            mask_ref[rows][None, :].astype(jnp.float32), (LANES, LANES)
        ).T
        lane = lax.broadcasted_iota(jnp.int32, (LANES, LANES), 1)
        raw = [
            prior_ref[rows, at : at + LANES] + jnp.where(label == lane + at, boost, 0.0)
            for at in range(0, classes, LANES)
        ]
        raw = jnp.concatenate(raw, axis=1)
        anchor = raw * (classes / jnp.sum(raw, axis=1, keepdims=True))
        anchor_ref[rows, :] = anchor
        for i, s in enumerate(sent_refs):
            s[rows, :] = anchor[:, i * width : (i + 1) * width].astype(jnp.bfloat16)


def prepare(label_prior, seed_label, seed_mask):
    nodes, classes = label_prior.shape
    sent = jax.ShapeDtypeStruct((nodes, classes // PARTS), jnp.bfloat16)
    anchor, *sent = pl.pallas_call(
        prepare_kernel,
        out_shape=[jax.ShapeDtypeStruct((nodes, classes), jnp.float32)] + [sent] * PARTS,
        in_specs=[VMEM, VMEM, VMEM],
        out_specs=[VMEM] * (1 + PARTS),
        cost_estimate=pl.CostEstimate(
            flops=8 * nodes * classes, bytes_accessed=10 * nodes * classes, transcendentals=0
        ),
        name="prepare",
    )(label_prior, seed_label, seed_mask)
    return anchor, sent


def reply_kernel(asked_ref, *refs, n_cols):
    parts, out_ref, table, in_sems, out_sem = refs[:n_cols], refs[n_cols], *refs[n_cols + 1 :]
    blocks_dev = parts[0].shape[0]
    n = out_ref.shape[0]
    loads = [
        pltpu.make_async_copy(p, table.at[pl.ds(i * blocks_dev, blocks_dev)], in_sems.at[i])
        for i, p in enumerate(parts)
    ]
    for c in loads:
        c.start()
    for c in loads:
        c.wait()

    @pl.loop(0, n // 2)
    def _(chip):
        for core in range(2):
            pltpu.make_async_copy(
                table.at[asked_ref[chip, core]], out_ref.at[2 * chip + core], out_sem
            ).start()

    pltpu.make_async_copy(out_ref, out_ref, out_sem).wait()


def reply_blocks(asked, parts):
    blocks_dev, block, width = parts[0].shape
    n = 2 * asked.shape[0]
    n_cols = len(parts)
    size = block * width * 2
    return pl.pallas_call(
        functools.partial(reply_kernel, n_cols=n_cols),
        out_shape=jax.ShapeDtypeStruct((n, block, width), jnp.bfloat16),
        in_specs=[SMEM] + [HBM] * n_cols,
        out_specs=ANY,
        scratch_shapes=[
            pltpu.VMEM((n_cols * blocks_dev, block, width), jnp.bfloat16),
            pltpu.SemaphoreType.DMA((n_cols,)),
            pltpu.SemaphoreType.DMA,
        ],
        cost_estimate=pl.CostEstimate(
            flops=4_000_000, bytes_accessed=(n + n_cols * blocks_dev) * size, transcendentals=0
        ),
        name="reply",
    )(asked, *parts)


def hold_kernel(turns_ref, *refs):
    spun = refs[-1]

    @pl.loop(0, turns_ref[0])
    def _(_):
        spun[...] = spun[...] * 0.5 + 1.0


def held(value, turns, after):
    return pl.pallas_call(
        hold_kernel,
        out_shape=jax.ShapeDtypeStruct(value.shape, value.dtype),
        in_specs=[SMEM, HBM] + [HBM] * len(after),
        out_specs=HBM,
        input_output_aliases={1: 0},
        scratch_shapes=[pltpu.VMEM((8, LANES), jnp.float32)],
        name="hold",
    )(turns, value, *after)


def spread_kernel(index_ref, core_ref, tiles_ref, weight_ref, anchor_ref, *refs, n_src, final):
    sources = [s if len(s.shape) == 3 else s.at[:, core_ref[0]] for s in refs[:n_src]]
    first_ref = refs[n_src] if final else None
    out_ref, table, sems = refs[-3:]
    blocks_dev, degree, block, _ = tiles_ref.shape
    width = anchor_ref.shape[1]
    loads, at = [], 0
    for i, s in enumerate(sources):
        loads.append(pltpu.make_async_copy(s, table.at[pl.ds(at, s.shape[0])], sems.at[i]))
        at += s.shape[0]
    for c in loads:
        c.start()
    for c in loads:
        c.wait()

    def row_block(b):
        left = jnp.concatenate([tiles_ref[b, k] for k in range(degree)], axis=1)
        right = jnp.concatenate(
            [table[index_ref[b * degree + k]] for k in range(degree)], axis=0
        )
        total = jnp.dot(left, right, preferred_element_type=jnp.float32)
        rows = pl.ds(b * block if final else pl.multiple_of(b * block, block), block)
        blended = weight_ref[rows, :] * total + anchor_ref[rows, :]
        if not final:
            out_ref[rows, :] = blended.astype(out_ref.dtype)
        else:
            first = first_ref[rows, :]
            classes = 2 * width
            factor = classes / jnp.sum(first + blended, axis=1, keepdims=True)
            out_ref[rows, :width] = first * factor
            out_ref[rows, width:] = blended * factor

    if final:
        for b in range(blocks_dev):
            row_block(b)
    else:
        pl.loop(0, blocks_dev)(row_block)


def spread_blocks(index, core, tiles, weight, anchor, sources, dtype, first=None):
    blocks_dev, degree, block, _ = tiles.shape
    width = anchor.shape[1]
    final = first is not None
    n_src = len(sources)
    total = sum(s.shape[0] for s in sources)
    places = [ANY if len(s.shape) == 3 else HBM for s in sources]
    return pl.pallas_call(
        functools.partial(spread_kernel, n_src=n_src, final=final),
        out_shape=jax.ShapeDtypeStruct((blocks_dev * block, width * (2 if final else 1)), dtype),
        in_specs=[SMEM, SMEM, VMEM, VMEM, VMEM] + places + [VMEM] * final,
        out_specs=VMEM,
        scratch_shapes=[
            pltpu.VMEM((total, block, width), jnp.bfloat16),
            pltpu.SemaphoreType.DMA((n_src,)),
        ],
        cost_estimate=pl.CostEstimate(
            flops=2 * blocks_dev * degree * block * block * width,
            bytes_accessed=total * block * width * 2 + tiles.size * 2,
            transcendentals=0,
        ),
        name="spread",
    )(index, core, tiles, weight, anchor, *sources, *([first] if final else []))


def local(adjacency_tiles, col_block, label_prior, seed_label, seed_mask):
    blocks_dev, _, block, _ = adjacency_tiles.shape
    classes = label_prior.shape[1]
    width = classes // PARTS
    n_rows = lax.axis_size(GROUP)
    n_cols = lax.axis_size("x")
    n_chips = lax.axis_size("zy")
    group_size = n_cols * blocks_dev
    own_group = lax.axis_index(GROUP)
    own_col = lax.axis_index("x")
    own_core = lax.axis_index("core")
    owner_group = col_block // group_size
    within = col_block % group_size

    place = (within // blocks_dev + n_cols - own_col) % n_cols * blocks_dev + within % blocks_dev
    chip, core = owner_group // 2, owner_group % 2
    slot = group_size + chip + jnp.where(core == own_core, 0, n_chips)
    index = jnp.where(owner_group == own_group, place, slot).reshape(-1)
    index_last = jnp.where(owner_group == own_group, place, group_size + owner_group).reshape(-1)
    asked = ask_blocks(owner_group, place, own_group, n_rows)
    anchor, blended = prepare(label_prior, seed_label, seed_mask)

    row_sum = jnp.sum(adjacency_tiles.astype(jnp.float32), axis=(1, 3)).reshape(-1, 1)
    scale = 1.0 / (ALPHA * row_sum + (1.0 - ALPHA))
    weight = jnp.broadcast_to(ALPHA * scale, (blocks_dev * block, width))

    ranges = [slice(p * width, (p + 1) * width) for p in range(PARTS)]
    anchors = [(1.0 - ALPHA) * scale * anchor[:, r] for r in ranges]
    before = []
    for hop in range(HOPS):
        last = hop == HOPS - 1
        for p in range(PARTS):
            own = blended[p].reshape(blocks_dev, block, width)
            pieces = [own] + [
                lax.ppermute(own, "x", [((x + d) % n_cols, x) for x in range(n_cols)])
                for d in range(1, n_cols)
            ]
            reply = reply_blocks(asked, pieces)
            if (hop, p) in HOLD:
                reply = held(reply, (own_core * HOLD[hop, p]).reshape(1), before)
            if last and p == PARTS - 1:
                remote = [lax.all_to_all(reply, GROUP, 0, 0, tiled=True)]
            else:
                reply = reply.reshape(n_chips, 2, block, width)
                same = lax.all_to_all(reply, "zy", 0, 0, tiled=True)
                before = [same]
                remote = [same, lax.ppermute(same, "core", [(0, 1), (1, 0)])]
            blended[p] = spread_blocks(
                index_last if len(remote) == 1 else index,
                own_core.reshape(1), adjacency_tiles, weight, anchors[p], pieces + remote,
                jnp.float32 if last else jnp.bfloat16,
                blended[0] if last and p == PARTS - 1 else None,
            )
    return blended[1]


def solution(mesh):
    n_rows, n_cols = mesh.devices.shape
    fine = Mesh(mesh.devices.reshape(n_rows // 2, 2, n_cols), AXES)
    in_specs = (
        P(AXES, None, None, None),
        P(AXES, None),
        P(AXES, None),
        P(AXES),
        P(AXES),
    )
    out_specs = P(AXES, None)

    return jax.shard_map(local, mesh=fine, in_specs=in_specs, out_specs=out_specs, check_vma=False)
```

```python
import functools

import jax
import jax.numpy as jnp
from jax import lax
from jax.experimental import pallas as pl
from jax.experimental.pallas import tpu as pltpu
from jax.sharding import Mesh
from jax.sharding import PartitionSpec as P

HOPS = 4
HOLD = {(0, 0): 2100, (1, 0): 700, (1, 1): 600, (2, 0): 700, (2, 1): 600, (3, 0): 700}
PARTS = 2
AXES = ("zy", "core", "x")
GROUP = ("zy", "core")
LANES = 128


ALPHA = 0.85
SEED_BOOST = 8.0

ANY = pl.BlockSpec(memory_space=pl.ANY)
VMEM = pl.BlockSpec(memory_space=pltpu.VMEM)
SMEM = pl.BlockSpec(memory_space=pltpu.SMEM)
HBM = pl.BlockSpec(memory_space=pltpu.HBM)


def ask_blocks(owner_group, place, own_group, n_rows):
    group_ids = jnp.arange(n_rows, dtype=jnp.int32)
    matched = owner_group.reshape(-1)[:, None] == group_ids[None, :]
    wanted = jnp.max(jnp.where(matched, place.reshape(-1)[:, None], 0), axis=0)
    wanted = jnp.where(group_ids == own_group, 0, wanted).reshape(n_rows // 2, 2)
    own_core = lax.axis_index("core")
    other = lax.ppermute(wanted, "core", [(0, 1), (1, 0)])
    lane = jnp.arange(LANES, dtype=jnp.int32)[None, :]
    mine = jnp.where(own_core == 0, wanted[:, :1], wanted[:, 1:])
    others = jnp.where(own_core == 0, other[:, :1], other[:, 1:])
    rows = jnp.where(lane % 2 == own_core, mine, others)
    return lax.all_to_all(rows, "zy", 0, 0, tiled=True)


def prepare_kernel(prior_ref, label_ref, mask_ref, anchor_ref, *sent_refs):
    nodes, classes = prior_ref.shape
    width = sent_refs[0].shape[1]

    @pl.loop(0, nodes // LANES)
    def _(b):
        rows = pl.ds(pl.multiple_of(b * LANES, LANES), LANES)
        label = jnp.broadcast_to(label_ref[rows][None, :], (LANES, LANES)).T
        boost = SEED_BOOST * jnp.broadcast_to(
            mask_ref[rows][None, :].astype(jnp.float32), (LANES, LANES)
        ).T
        lane = lax.broadcasted_iota(jnp.int32, (LANES, LANES), 1)
        raw = [
            prior_ref[rows, at : at + LANES] + jnp.where(label == lane + at, boost, 0.0)
            for at in range(0, classes, LANES)
        ]
        raw = jnp.concatenate(raw, axis=1)
        anchor = raw * (classes / jnp.sum(raw, axis=1, keepdims=True))
        anchor_ref[rows, :] = anchor
        for i, s in enumerate(sent_refs):
            s[rows, :] = anchor[:, i * width : (i + 1) * width].astype(jnp.bfloat16)


def prepare(label_prior, seed_label, seed_mask):
    nodes, classes = label_prior.shape
    sent = jax.ShapeDtypeStruct((nodes, classes // PARTS), jnp.bfloat16)
    anchor, *sent = pl.pallas_call(
        prepare_kernel,
        out_shape=[jax.ShapeDtypeStruct((nodes, classes), jnp.float32)] + [sent] * PARTS,
        in_specs=[VMEM, VMEM, VMEM],
        out_specs=[VMEM] * (1 + PARTS),
        cost_estimate=pl.CostEstimate(
            flops=8 * nodes * classes, bytes_accessed=10 * nodes * classes, transcendentals=0
        ),
        name="prepare",
    )(label_prior, seed_label, seed_mask)
    return anchor, sent


def reply_kernel(asked_ref, *refs, n_cols):
    parts, out_ref, table, in_sems, out_sem = refs[:n_cols], refs[n_cols], *refs[n_cols + 1 :]
    blocks_dev = parts[0].shape[0]
    n = out_ref.shape[0]
    loads = [
        pltpu.make_async_copy(p, table.at[pl.ds(i * blocks_dev, blocks_dev)], in_sems.at[i])
        for i, p in enumerate(parts)
    ]
    for c in loads:
        c.start()
    for c in loads:
        c.wait()

    @pl.loop(0, n // 2)
    def _(chip):
        for core in range(2):
            pltpu.make_async_copy(
                table.at[asked_ref[chip, core]], out_ref.at[2 * chip + core], out_sem
            ).start()

    pltpu.make_async_copy(out_ref, out_ref, out_sem).wait()


def reply_blocks(asked, parts):
    blocks_dev, block, width = parts[0].shape
    n = 2 * asked.shape[0]
    n_cols = len(parts)
    size = block * width * 2
    return pl.pallas_call(
        functools.partial(reply_kernel, n_cols=n_cols),
        out_shape=jax.ShapeDtypeStruct((n, block, width), jnp.bfloat16),
        in_specs=[SMEM] + [HBM] * n_cols,
        out_specs=ANY,
        scratch_shapes=[
            pltpu.VMEM((n_cols * blocks_dev, block, width), jnp.bfloat16),
            pltpu.SemaphoreType.DMA((n_cols,)),
            pltpu.SemaphoreType.DMA,
        ],
        cost_estimate=pl.CostEstimate(
            flops=4_000_000, bytes_accessed=(n + n_cols * blocks_dev) * size, transcendentals=0
        ),
        name="reply",
    )(asked, *parts)


def hold_kernel(turns_ref, *refs):
    spun = refs[-1]

    @pl.loop(0, turns_ref[0])
    def _(_):
        spun[...] = spun[...] * 0.5 + 1.0


def held(value, turns, after):
    return pl.pallas_call(
        hold_kernel,
        out_shape=jax.ShapeDtypeStruct(value.shape, value.dtype),
        in_specs=[SMEM, HBM] + [HBM] * len(after),
        out_specs=HBM,
        input_output_aliases={1: 0},
        scratch_shapes=[pltpu.VMEM((8, LANES), jnp.float32)],
        name="hold",
    )(turns, value, *after)


def spread_kernel(index_ref, core_ref, tiles_ref, weight_ref, anchor_ref, *refs, n_src, final):
    sources = [s if len(s.shape) == 3 else s.at[:, core_ref[0]] for s in refs[:n_src]]
    first_ref = refs[n_src] if final else None
    out_ref, table, sems = refs[-3:]
    blocks_dev, degree, block, _ = tiles_ref.shape
    width = anchor_ref.shape[1]
    loads, at = [], 0
    for i, s in enumerate(sources):
        loads.append(pltpu.make_async_copy(s, table.at[pl.ds(at, s.shape[0])], sems.at[i]))
        at += s.shape[0]
    for c in loads:
        c.start()
    for c in loads:
        c.wait()

    def row_block(b):
        left = jnp.concatenate([tiles_ref[b, k] for k in range(degree)], axis=1)
        right = jnp.concatenate(
            [table[index_ref[b * degree + k]] for k in range(degree)], axis=0
        )
        total = jnp.dot(left, right, preferred_element_type=jnp.float32)
        rows = pl.ds(b * block if final else pl.multiple_of(b * block, block), block)
        blended = weight_ref[rows, :] * total + anchor_ref[rows, :]
        if not final:
            out_ref[rows, :] = blended.astype(out_ref.dtype)
        else:
            first = first_ref[rows, :]
            classes = 2 * width
            factor = classes / jnp.sum(first + blended, axis=1, keepdims=True)
            out_ref[rows, :width] = first * factor
            out_ref[rows, width:] = blended * factor

    if final:
        for b in range(blocks_dev):
            row_block(b)
    else:
        pl.loop(0, blocks_dev)(row_block)


def spread_blocks(index, core, tiles, weight, anchor, sources, dtype, first=None):
    blocks_dev, degree, block, _ = tiles.shape
    width = anchor.shape[1]
    final = first is not None
    n_src = len(sources)
    total = sum(s.shape[0] for s in sources)
    places = [ANY if len(s.shape) == 3 else HBM for s in sources]
    return pl.pallas_call(
        functools.partial(spread_kernel, n_src=n_src, final=final),
        out_shape=jax.ShapeDtypeStruct((blocks_dev * block, width * (2 if final else 1)), dtype),
        in_specs=[SMEM, SMEM, VMEM, VMEM, VMEM] + places + [VMEM] * final,
        out_specs=VMEM,
        scratch_shapes=[
            pltpu.VMEM((total, block, width), jnp.bfloat16),
            pltpu.SemaphoreType.DMA((n_src,)),
        ],
        cost_estimate=pl.CostEstimate(
            flops=2 * blocks_dev * degree * block * block * width,
            bytes_accessed=total * block * width * 2 + tiles.size * 2,
            transcendentals=0,
        ),
        name="spread",
    )(index, core, tiles, weight, anchor, *sources, *([first] if final else []))


def local(adjacency_tiles, col_block, label_prior, seed_label, seed_mask):
    blocks_dev, _, block, _ = adjacency_tiles.shape
    classes = label_prior.shape[1]
    width = classes // PARTS
    n_rows = lax.axis_size(GROUP)
    n_cols = lax.axis_size("x")
    n_chips = lax.axis_size("zy")
    group_size = n_cols * blocks_dev
    own_group = lax.axis_index(GROUP)
    own_col = lax.axis_index("x")
    own_core = lax.axis_index("core")
    owner_group = col_block // group_size
    within = col_block % group_size

    place = (within // blocks_dev + n_cols - own_col) % n_cols * blocks_dev + within % blocks_dev
    chip, core = owner_group // 2, owner_group % 2
    slot = group_size + chip + jnp.where(core == own_core, 0, n_chips)
    index = jnp.where(owner_group == own_group, place, slot).reshape(-1)
    asked = ask_blocks(owner_group, place, own_group, n_rows)
    anchor, blended = prepare(label_prior, seed_label, seed_mask)

    row_sum = jnp.sum(adjacency_tiles.astype(jnp.float32), axis=(1, 3)).reshape(-1, 1)
    scale = 1.0 / (ALPHA * row_sum + (1.0 - ALPHA))
    weight = jnp.broadcast_to(ALPHA * scale, (blocks_dev * block, width))

    ranges = [slice(p * width, (p + 1) * width) for p in range(PARTS)]
    anchors = [(1.0 - ALPHA) * scale * anchor[:, r] for r in ranges]
    before = []
    for hop in range(HOPS):
        last = hop == HOPS - 1
        for p in range(PARTS):
            own = blended[p].reshape(blocks_dev, block, width)
            pieces = [own] + [
                lax.ppermute(own, "x", [((x + d) % n_cols, x) for x in range(n_cols)])
                for d in range(1, n_cols)
            ]
            reply = reply_blocks(asked, pieces)
            if (hop, p) in HOLD:
                reply = held(reply, (own_core * HOLD[hop, p]).reshape(1), before)
            reply = reply.reshape(n_chips, 2, block, width)
            same = lax.all_to_all(reply, "zy", 0, 0, tiled=True)
            before = [same]
            remote = [same, lax.ppermute(same, "core", [(0, 1), (1, 0)])]
            blended[p] = spread_blocks(
                index,
                own_core.reshape(1), adjacency_tiles, weight, anchors[p], pieces + remote,
                jnp.float32 if last else jnp.bfloat16,
                blended[0] if last and p == PARTS - 1 else None,
            )
    return blended[1]


def solution(mesh):
    n_rows, n_cols = mesh.devices.shape
    fine = Mesh(mesh.devices.reshape(n_rows // 2, 2, n_cols), AXES)
    in_specs = (
        P(AXES, None, None, None),
        P(AXES, None),
        P(AXES, None),
        P(AXES),
        P(AXES),
    )
    out_specs = P(AXES, None)

    return jax.shard_map(local, mesh=fine, in_specs=in_specs, out_specs=out_specs, check_vma=False)
```
